8 devices in a mesh: data: 8 (over z, y, x, core).
Axes of the slice: x: 2, y: 2, z: 1, core: 2. Of those that a mesh axis runs over, the one named last changes fastest.
Arguments:
- act_in: bfloat16 [8192, 1536], P('data')
- grad_out: bfloat16 [8192, 1536], P('data')
- w_up: bfloat16 [2, 1536, 8960], replicated
- w_down: bfloat16 [2, 8960, 1536], replicated
- master_up: float32 [2, 1536, 8960], P(None, 'data')
- master_down: float32 [2, 8960, 1536], P(None, 'data')
- exp_avg_up: float32 [2, 1536, 8960], P(None, 'data')
- exp_avg_down: float32 [2, 8960, 1536], P(None, 'data')
- exp_sq_up: float32 [2, 1536, 8960], P(None, 'data')
- exp_sq_down: float32 [2, 8960, 1536], P(None, 'data')
- learn_rate: float32 [], replicated
- clip_norm: float32 [], replicated
Outputs:
- output 1: bfloat16 [2, 1536, 8960], replicated
- output 2: bfloat16 [2, 8960, 1536], replicated
- output 3: float32 [2, 1536, 8960], P(None, 'data')
- output 4: float32 [2, 8960, 1536], P(None, 'data')
- output 5: float32 [2, 1536, 8960], P(None, 'data')
- output 6: float32 [2, 8960, 1536], P(None, 'data')
- output 7: float32 [2, 1536, 8960], P(None, 'data')
- output 8: float32 [2, 8960, 1536], P(None, 'data')
- output 9: float32 [], replicated
All inputs are finite; a program needn't handle non-finite values.
Results may differ from the reference program's by a relative error of at most 0.00439.
Values are sent between devices in bfloat16 or wider.
A program may use at most 1.5 GiB of HBM per device.

```python
import jax
import jax.numpy as jnp
from jax import lax

D = 1536
FF = 8960
TOKENS_DEV = 1024
GROUP = 8
STEP = 10

BETA_ONE = 0.9
BETA_TWO = 0.95
ADAM_EPS = 1e-8
NORM_EPS = 1e-6
INV_SQRT_TWO = 0.7071067811865476
INV_SQRT_TWO_PI = 0.3989422804014327


def gelu_parts(pre_act):
    normal_cdf = 0.5 * (1.0 + lax.erf(pre_act * INV_SQRT_TWO))
    normal_pdf = jnp.exp(-0.5 * pre_act * pre_act) * INV_SQRT_TWO_PI
    return pre_act * normal_cdf, normal_cdf + pre_act * normal_pdf


def block_grads(act_blk, out_blk, w_up, w_down):
    z_one = jnp.dot(act_blk, w_up[0], preferred_element_type=jnp.float32)
    gelu_one, slope_one = gelu_parts(z_one)
    act_one = gelu_one.astype(jnp.bfloat16)
    hidden = jnp.dot(act_one, w_down[0], preferred_element_type=jnp.float32).astype(jnp.bfloat16)
    z_three = jnp.dot(hidden, w_up[1], preferred_element_type=jnp.float32)
    gelu_three, slope_three = gelu_parts(z_three)
    act_three = gelu_three.astype(jnp.bfloat16)
    g_four = jnp.dot(act_three.T, out_blk, preferred_element_type=jnp.float32)
    dz_three = (jnp.dot(out_blk, w_down[1].T, preferred_element_type=jnp.float32) * slope_three).astype(jnp.bfloat16)
    g_three = jnp.dot(hidden.T, dz_three, preferred_element_type=jnp.float32)
    d_hidden = jnp.dot(dz_three, w_up[1].T, preferred_element_type=jnp.float32).astype(jnp.bfloat16)
    g_two = jnp.dot(act_one.T, d_hidden, preferred_element_type=jnp.float32)
    dz_one = (jnp.dot(d_hidden, w_down[0].T, preferred_element_type=jnp.float32) * slope_one).astype(jnp.bfloat16)
    g_one = jnp.dot(act_blk.T, dz_one, preferred_element_type=jnp.float32)
    return jnp.stack([g_one, g_three]), jnp.stack([g_two, g_four])


def full_grads(act_in, grad_out, w_up, w_down):
    act_blocks = act_in.reshape(GROUP, TOKENS_DEV, D)
    out_blocks = grad_out.reshape(GROUP, TOKENS_DEV, D)

    def add_block(carry_sums, blocks):
        grad_up, grad_down = block_grads(blocks[0], blocks[1], w_up, w_down)
        return (carry_sums[0] + grad_up, carry_sums[1] + grad_down), None

    start_sums = (jnp.zeros((2, D, FF), jnp.float32), jnp.zeros((2, FF, D), jnp.float32))
    final_sums = lax.scan(add_block, start_sums, (act_blocks, out_blocks))[0]
    return final_sums[0] / GROUP, final_sums[1] / GROUP


def lamb_update(master, exp_avg, exp_sq, grad, clip_scale, learn_rate):
    bias_one = 1.0 - BETA_ONE ** STEP
    bias_two = 1.0 - BETA_TWO ** STEP
    avg_new = BETA_ONE * exp_avg + (1.0 - BETA_ONE) * clip_scale * grad
    sq_new = BETA_TWO * exp_sq + (1.0 - BETA_TWO) * (clip_scale * clip_scale) * (grad * grad)
    direction = (avg_new / bias_one) / (jnp.sqrt(sq_new / bias_two) + ADAM_EPS)
    master_norm = jnp.sqrt(jnp.sum(master * master, axis=(1, 2), keepdims=True))
    dir_norm = jnp.sqrt(jnp.sum(direction * direction, axis=(1, 2), keepdims=True))
    master_new = master - learn_rate * (master_norm / dir_norm) * direction
    return master_new, avg_new, sq_new


def row_profile(key, row_count, spread):
    walk = jnp.cumsum(jax.random.normal(key, (row_count,), jnp.float32)) / (row_count ** 0.5)
    return jnp.exp(spread * (walk - jnp.mean(walk)))


def setup_inputs(seed: int = 0) -> dict:
    keys = jax.random.split(jax.random.key(seed), 24)
    row_total = TOKENS_DEV * GROUP
    init_scale = D ** -0.5
    out_scale = (GROUP / TOKENS_DEV) ** 0.5
    act_in = jax.random.normal(keys[0], (row_total, D), jnp.float32).astype(jnp.bfloat16)
    grad_out = (jax.random.normal(keys[1], (row_total, D), jnp.float32) * out_scale).astype(jnp.bfloat16)
    prof_up = jnp.stack([row_profile(keys[2], D, 0.7), row_profile(keys[3], D, 0.7)])[:, :, None]
    prof_down = jnp.stack([row_profile(keys[4], FF, 0.7), row_profile(keys[5], FF, 0.7)])[:, :, None]
    base_up = jax.random.normal(keys[6], (2, D, FF), jnp.float32) * init_scale * prof_up
    base_down = jax.random.normal(keys[7], (2, FF, D), jnp.float32) * init_scale * prof_down
    w_up = base_up.astype(jnp.bfloat16)
    w_down = base_down.astype(jnp.bfloat16)
    master_up = base_up + 0.02 * init_scale * prof_up * jax.random.normal(keys[8], (2, D, FF), jnp.float32)
    master_down = base_down + 0.02 * init_scale * prof_down * jax.random.normal(keys[9], (2, FF, D), jnp.float32)
    grad_up, grad_down = full_grads(act_in, grad_out, w_up, w_down)
    grad_norm = jnp.sqrt(jnp.sum(grad_up * grad_up) + jnp.sum(grad_down * grad_down))
    clip_norm = jax.random.uniform(keys[10], (), jnp.float32, 0.3, 0.7) * grad_norm
    clip_scale = clip_norm / (grad_norm + NORM_EPS)
    step_up = clip_scale * jnp.sqrt(jnp.mean(grad_up * grad_up, axis=(1, 2), keepdims=True))
    step_down = clip_scale * jnp.sqrt(jnp.mean(grad_down * grad_down, axis=(1, 2), keepdims=True))
    exp_avg_up = 0.1 * step_up * jax.random.normal(keys[11], (2, D, FF), jnp.float32)
    exp_avg_down = 0.1 * step_down * jax.random.normal(keys[12], (2, FF, D), jnp.float32)
    sq_prof_up = jnp.stack([row_profile(keys[13], D, 1.5), row_profile(keys[14], D, 1.5)])[:, :, None]
    sq_prof_down = jnp.stack([row_profile(keys[15], FF, 1.5), row_profile(keys[16], FF, 1.5)])[:, :, None]
    exp_sq_up = 0.05 * step_up * step_up * sq_prof_up * jax.random.uniform(keys[17], (2, D, FF), jnp.float32, 0.5, 1.5)
    exp_sq_down = 0.05 * step_down * step_down * sq_prof_down * jax.random.uniform(keys[18], (2, FF, D), jnp.float32, 0.5, 1.5)
    learn_rate = jax.random.uniform(keys[19], (), jnp.float32, 0.08, 0.16)
    return {"act_in": act_in, "grad_out": grad_out, "w_up": w_up, "w_down": w_down, "master_up": master_up, "master_down": master_down, "exp_avg_up": exp_avg_up, "exp_avg_down": exp_avg_down, "exp_sq_up": exp_sq_up, "exp_sq_down": exp_sq_down, "learn_rate": learn_rate, "clip_norm": clip_norm}


def reference(act_in, grad_out, w_up, w_down, master_up, master_down, exp_avg_up, exp_avg_down, exp_sq_up, exp_sq_down, learn_rate, clip_norm):
    grad_up, grad_down = full_grads(act_in, grad_out, w_up, w_down)
    grad_norm = jnp.sqrt(jnp.sum(grad_up * grad_up) + jnp.sum(grad_down * grad_down))
    clip_scale = jnp.minimum(1.0, clip_norm / (grad_norm + NORM_EPS))
    master_up_out, avg_up, sq_up = lamb_update(master_up, exp_avg_up, exp_sq_up, grad_up, clip_scale, learn_rate)
    master_down_out, avg_down, sq_down = lamb_update(master_down, exp_avg_down, exp_sq_down, grad_down, clip_scale, learn_rate)
    return (master_up_out.astype(jnp.bfloat16), master_down_out.astype(jnp.bfloat16), master_up_out, master_down_out, avg_up, avg_down, sq_up, sq_down, grad_norm)
```

```python
import functools

import jax
import jax.numpy as jnp
from jax import lax
from jax.experimental import pallas as pl
from jax.experimental.pallas import tpu as pltpu
from jax.sharding import PartitionSpec as P


STEP = 10
BETA_ONE = 0.9
BETA_TWO = 0.95
ADAM_EPS = 1e-8
NORM_EPS = 1e-6
INV_SQRT_TWO = 0.7071067811865476
INV_SQRT_TWO_PI = 0.3989422804014327
INV_BIAS_ONE = 1.0 / (1.0 - BETA_ONE ** STEP)
INV_BIAS_TWO = 1.0 / (1.0 - BETA_TWO ** STEP)

MESH = pl.DeviceIdType.MESH
ANY = pl.BlockSpec(memory_space=pl.ANY)
SMEM = pl.BlockSpec(memory_space=pltpu.SMEM)
BF = jnp.bfloat16


def gelu_val(pre_act):
    return pre_act * (0.5 * (1.0 + lax.erf(pre_act * INV_SQRT_TWO)))


def gelu_slope(pre_act):
    normal_cdf = 0.5 * (1.0 + lax.erf(pre_act * INV_SQRT_TWO))
    normal_pdf = jnp.exp(-0.5 * pre_act * pre_act) * INV_SQRT_TWO_PI
    return normal_cdf + pre_act * normal_pdf


def mm(spec, lhs, rhs):
    return jnp.einsum(spec, lhs, rhs, preferred_element_type=jnp.float32)


def params(mib=48, **kw):
    return pltpu.CompilerParams(vmem_limit_bytes=mib << 20, **kw)


def psum_kernel(n, x_ref, o_ref, buf, send_sem, recv_sem):
    me = lax.axis_index("data")
    barrier = pltpu.get_barrier_semaphore()
    for d in range(1, n):
        pl.semaphore_signal(barrier, inc=1, device_id=(lax.bitwise_xor(me, d),), device_id_type=MESH)
    pl.semaphore_wait(barrier, n - 1)
    copies = []
    for d in range(1, n):
        copy = pltpu.make_async_remote_copy(
            src_ref=x_ref, dst_ref=buf.at[me], send_sem=send_sem.at[d], recv_sem=recv_sem.at[d],
            device_id=(lax.bitwise_xor(me, d),), device_id_type=MESH)
        copy.start()
        copies.append(copy)
    buf[me] = x_ref[...]
    for copy in copies:
        copy.wait()
    total = buf[0]
    for d in range(1, n):
        total = total + buf[d]
    for k in range(x_ref.shape[0]):
        o_ref[k] = jnp.sum(total[k])


def device_sums(parts, n, collective_id):
    k = parts.shape[0]
    return pl.pallas_call(
        functools.partial(psum_kernel, n),
        out_shape=jax.ShapeDtypeStruct((k,), jnp.float32),
        in_specs=[pl.BlockSpec(memory_space=pltpu.VMEM)],
        out_specs=SMEM,
        scratch_shapes=[pltpu.VMEM((n, k, 8, 128), jnp.float32), pltpu.SemaphoreType.DMA((n,)), pltpu.SemaphoreType.DMA((n,))],
        compiler_params=pltpu.CompilerParams(collective_id=collective_id, has_side_effects=True),
    )(parts)


def direction(avg_new, sq_new):
    return (avg_new * INV_BIAS_ONE) / (jnp.sqrt(sq_new * INV_BIAS_TWO) + ADAM_EPS)


def fold(x):
    rows, cols = x.shape
    return jnp.sum(jnp.sum(x.reshape(rows // 8, 8, cols), axis=0).reshape(8, cols // 128, 128), axis=1)


def moments(s_ref, g, m_ref, v_ref, mo_ref, vo_ref, acc_ref, first):
    s = s_ref[0]
    m = BETA_ONE * m_ref[0] + ((1.0 - BETA_ONE) * s) * g
    v = BETA_TWO * v_ref[0] + ((1.0 - BETA_TWO) * (s * s)) * (g * g)
    mo_ref[0] = m
    vo_ref[0] = v
    u = direction(m, v)

    @pl.when(first)
    def _():
        acc_ref[...] = jnp.zeros_like(acc_ref)

    acc_ref[0] += fold(u * u)


def moments_down_kernel(s_ref, ga_ref, gb_ref, m_ref, v_ref, mo_ref, vo_ref, acc_ref):
    k = pl.program_id(0)
    g = jnp.where(k == 0, ga_ref[...], gb_ref[...])
    moments(s_ref, g, m_ref, v_ref, mo_ref, vo_ref, acc_ref, pl.program_id(1) == 0)


def moments_down(scale, g_a, g_b, m, v, rows):
    _, total, cols = m.shape
    blocks = total // rows
    state = pl.BlockSpec((1, rows, cols), lambda k, i: (k, i, 0))
    return pl.pallas_call(
        moments_down_kernel,
        grid=(2, blocks),
        out_shape=(jax.ShapeDtypeStruct(m.shape, m.dtype), jax.ShapeDtypeStruct(v.shape, v.dtype), jax.ShapeDtypeStruct((2, 8, 128), jnp.float32)),
        in_specs=[SMEM,
                  pl.BlockSpec((rows, cols), lambda k, i: (jnp.where(k == 0, i, blocks - 1), 0)),
                  pl.BlockSpec((rows, cols), lambda k, i: (jnp.where(k == 0, 0, i), 0)),
                  state, state],
        out_specs=(state, state, pl.BlockSpec((1, 8, 128), lambda k, i: (k, 0, 0))),
        compiler_params=params(),
        cost_estimate=pl.CostEstimate(flops=40 * m.size, bytes_accessed=20 * m.size, transcendentals=2 * m.size),
        name="moments_down",
    )(scale, g_a, g_b, m, v)


def moments_up_kernel(s_ref, g_ref, m_ref, v_ref, *rest):
    mo_ref, vo_ref, acc_ref, g_scr = rest[-4:]
    parts, _, width = g_ref.shape
    for p in range(parts):
        g_scr[:, p * width:(p + 1) * width] = g_ref[p]
    moments(s_ref, g_scr[...], m_ref, v_ref, mo_ref, vo_ref, acc_ref, pl.program_id(0) == 0)


def moments_up(scale, g_parts, m, v, which, into, rows):
    _, total, cols = m.shape
    n, _, width = g_parts.shape
    state = pl.BlockSpec((1, rows, cols), lambda i: (which, i, 0))
    extra = [] if into is None else list(into)
    return pl.pallas_call(
        moments_up_kernel,
        grid=(total // rows,),
        out_shape=(jax.ShapeDtypeStruct(m.shape, m.dtype), jax.ShapeDtypeStruct(v.shape, v.dtype), jax.ShapeDtypeStruct((1, 8, 128), jnp.float32)),
        in_specs=[SMEM, pl.BlockSpec((n, rows, width), lambda i: (0, i, 0)), state, state] + [ANY] * len(extra),
        out_specs=(state, state, pl.BlockSpec((1, 8, 128), lambda i: (0, 0, 0))),
        scratch_shapes=[pltpu.VMEM((rows, cols), jnp.float32)],
        input_output_aliases={} if into is None else {4: 0, 5: 1},
        compiler_params=params(),
        cost_estimate=pl.CostEstimate(flops=20 * m.size, bytes_accessed=10 * m.size, transcendentals=m.size),
    )(scale, g_parts, m, v, *extra)


def apply_kernel(f_ref, p_ref, m_ref, v_ref, *rest):
    po_ref, w_ref = rest[-2:]
    new = p_ref[0] - f_ref[0] * direction(m_ref[0], v_ref[0])
    po_ref[0] = new
    w_ref[...] = new.astype(w_ref.dtype)


def apply_update(factor, master, m, v, which, into, rows):
    _, total, cols = m.shape
    state = pl.BlockSpec((1, rows, cols), lambda i: (which, i, 0))
    extra = [] if into is None else [into]
    return pl.pallas_call(
        apply_kernel,
        grid=(total // rows,),
        out_shape=(jax.ShapeDtypeStruct(m.shape, m.dtype), jax.ShapeDtypeStruct((total, cols), BF)),
        in_specs=[SMEM, state, state, state] + [ANY] * len(extra),
        out_specs=(state, pl.BlockSpec((rows, cols), lambda i: (i, 0))),
        input_output_aliases={} if into is None else {4: 0},
        compiler_params=params(),
        cost_estimate=pl.CostEstimate(flops=15 * m.size, bytes_accessed=9 * m.size, transcendentals=m.size),
    )(factor, master, m, v, *extra)


def ag_kernel(count, *refs):
    ins, outs = refs[:count], refs[count:2 * count]
    send_sem, recv_sem, local_sem = refs[2 * count:]
    me = lax.axis_index("data")
    core, nx, ny, nd = (lax.bitwise_xor(me, b) for b in (1, 2, 4, 6))
    barrier = pltpu.get_barrier_semaphore()
    for peer in (core, nx, ny):
        pl.semaphore_signal(barrier, inc=1, device_id=(peer,), device_id_type=MESH)
    pl.semaphore_wait(barrier, 3)

    def rows(a, owner, half):
        height = ins[a].shape[0]
        first = (height // 2 + 15) // 16 * 16
        if half is None:
            return pl.ds(owner * height, height)
        start, size = (0, first) if half == 0 else (first, height - first)
        return pl.ds(owner * height + start, size)

    def own(a, half):
        height = ins[a].shape[0]
        first = (height // 2 + 15) // 16 * 16
        if half is None:
            return ins[a]
        return ins[a].at[pl.ds(0, first)] if half == 0 else ins[a].at[pl.ds(first, height - first)]

    def copy(a, slot, src, owner, half, peer):
        return pltpu.make_async_remote_copy(
            src_ref=src, dst_ref=outs[a].at[rows(a, owner, half)], send_sem=send_sem.at[a, slot], recv_sem=recv_sem.at[a, slot],
            device_id=(peer,), device_id_type=MESH)

    def held(a, owner, half):
        return outs[a].at[rows(a, owner, half)]

    arrays = range(count)
    local = [pltpu.make_async_copy(ins[a], held(a, me, None), local_sem.at[a]) for a in arrays]
    started = []

    def go(c):
        c.start()
        started.append(c)
        return c

    x_first = [go(copy(a, 0, own(a, 0), me, 0, nx)) for a in arrays]
    y_first = [go(copy(a, 1, own(a, 1), me, 1, ny)) for a in arrays]
    x_second = [go(copy(a, 2, own(a, 1), me, 1, nx)) for a in arrays]
    y_second = [go(copy(a, 3, own(a, 0), me, 0, ny)) for a in arrays]
    c_own = [go(copy(a, 4, ins[a], me, None, core)) for a in arrays]
    for c in local:
        c.start()
    y_third, x_third = [], []
    for a in arrays:
        x_first[a].wait_recv()
        y_third.append(go(copy(a, 5, held(a, nx, 0), nx, 0, ny)))
        go(copy(a, 7, held(a, nx, 0), nx, 0, core))
        y_first[a].wait_recv()
        x_third.append(go(copy(a, 6, held(a, ny, 1), ny, 1, nx)))
        go(copy(a, 8, held(a, ny, 1), ny, 1, core))
    for a in arrays:
        x_second[a].wait_recv()
        go(copy(a, 9, held(a, nx, 1), nx, 1, core))
        y_second[a].wait_recv()
        go(copy(a, 10, held(a, ny, 0), ny, 0, core))
    for a in arrays:
        y_third[a].wait_recv()
        go(copy(a, 11, held(a, nd, 0), nd, 0, core))
        x_third[a].wait_recv()
        go(copy(a, 12, held(a, nd, 1), nd, 1, core))
    for c in c_own:
        c.wait_recv()
    for c in started:
        c.wait_send()
    for a in arrays:
        for slot in range(7, 13):
            half = 0 if slot in (7, 10, 11) else 1
            copy(a, slot, held(a, me, half), me, half, core).wait_recv()
    for c in local:
        c.wait()


def gather_rows(shards, n, collective_id):
    count = len(shards)
    return pl.pallas_call(
        functools.partial(ag_kernel, count),
        out_shape=[jax.ShapeDtypeStruct((n * s.shape[0],) + s.shape[1:], s.dtype) for s in shards],
        in_specs=[ANY] * count,
        out_specs=[ANY] * count,
        scratch_shapes=[pltpu.SemaphoreType.DMA((count, 13)), pltpu.SemaphoreType.DMA((count, 13)), pltpu.SemaphoreType.DMA((count,))],
        compiler_params=pltpu.CompilerParams(collective_id=collective_id, has_side_effects=True),
        cost_estimate=pl.CostEstimate(flops=0, bytes_accessed=2 * n * sum(s.size for s in shards), transcendentals=0),
    )(*shards)


def place_kernel(x_ref, *rest):
    rest[-1][0] = x_ref[...]


def place(x, which, into, rows):
    total, cols = x.shape
    extra = [] if into is None else [into]
    return pl.pallas_call(
        place_kernel,
        grid=(total // rows,),
        out_shape=jax.ShapeDtypeStruct((2, total, cols), x.dtype),
        in_specs=[pl.BlockSpec((rows, cols), lambda i: (i, 0))] + [ANY] * len(extra),
        out_specs=pl.BlockSpec((1, rows, cols), lambda i: (which, i, 0)),
        input_output_aliases={} if into is None else {1: 0},
        compiler_params=params(),
        cost_estimate=pl.CostEstimate(flops=x.size, bytes_accessed=4 * x.size, transcendentals=0),
    )(x, *extra)


def solution(mesh):
    n = mesh.shape["data"]
    batch_rows = P("data", None)
    state_rows = P(None, "data", None)
    replicated = P()

    def gather(x):
        return lax.all_gather(x, "data", axis=0, tiled=True)

    def device_body(act_in, grad_out, w_up, w_down, master_up, master_down, exp_avg_up, exp_avg_down, exp_sq_up, exp_sq_down, learn_rate, clip_norm):
        dim, ff = w_up.shape[1:]
        fs, ds = ff // n, dim // n
        me = lax.axis_index("data")
        e_all = gather(grad_out)
        x_all = gather(act_in)
        master_sq = jnp.concatenate([jnp.sum(master_up * master_up, axis=(1, 2)), jnp.sum(master_down * master_down, axis=(1, 2))])
        act_one = gelu_val(mm("td,df->tf", act_in, w_up[0])).astype(BF)
        hidden = mm("tf,fd->td", act_one, w_down[0]).astype(BF)
        h_all = gather(hidden)
        z_three = mm("td,df->tf", hidden, w_up[1])
        dz_three = (mm("td,fd->tf", grad_out, w_down[1]) * gelu_slope(z_three)).astype(BF)
        d_hidden = mm("tf,df->td", dz_three, w_up[1]).astype(BF)
        r_all = gather(d_hidden)
        up_slice = lax.dynamic_slice(w_up, (0, 0, me * fs), (2, dim, fs))
        down_slice = lax.dynamic_slice(w_down, (0, me * fs, 0), (2, fs, dim))

        def pair(x_in, up, down, cot):
            z = mm("df,td->ft", up, x_in)
            act = gelu_val(z).astype(BF)
            q = (mm("fd,td->ft", down, cot) * gelu_slope(z)).astype(BF)
            g_up = mm("td,ft->df", x_in, q) / n
            g_down = mm("ft,td->fd", act, cot) / n
            return g_up, g_down

        def exchange(g_up):
            return lax.all_to_all(g_up.reshape(n, ds, fs), "data", split_axis=0, concat_axis=0, tiled=False)

        g_three, g_four = pair(h_all, up_slice[1], down_slice[1], e_all)
        parts_three = exchange(g_three)
        g_one, g_two = pair(x_all, up_slice[0], down_slice[0], r_all)
        parts_one = exchange(g_one)
        local_sq = sum(jnp.sum(g * g) for g in (g_one, g_two, g_three, g_four))

        def tile(x):
            return jnp.where((lax.broadcasted_iota(jnp.int32, (8, 128), 0) + lax.broadcasted_iota(jnp.int32, (8, 128), 1)) == 0, x, 0.0)[None]

        grad_norm = jnp.sqrt(device_sums(tile(local_sq), n, 1)[0])
        scale = jnp.minimum(1.0, clip_norm / (grad_norm + NORM_EPS)).reshape(1)
        avg_down, sq_down, stat_down = moments_down(scale, g_two, g_four, exp_avg_down, exp_sq_down, 160)
        avg_up, sq_up, stat_three = moments_up(scale, parts_three, exp_avg_up, exp_sq_up, 1, None, 32)
        early = device_sums(jnp.concatenate([stat_down, stat_three, tile(master_sq[0]), tile(master_sq[1]), tile(master_sq[2]), tile(master_sq[3])]), n, 2)
        factor = lambda master_total, dir_total: (learn_rate * (jnp.sqrt(master_total) / jnp.sqrt(dir_total))).reshape(1)
        master_down_out, own_two = apply_update(factor(early[5], early[0]), master_down, avg_down, sq_down, 0, None, 160)
        new_two = gather(own_two)
        avg_up, sq_up, stat_one = moments_up(scale, parts_one, exp_avg_up, exp_sq_up, 0, (avg_up, sq_up), 32)
        late = device_sums(stat_one, n, 3)
        master_down_out, own_four = apply_update(factor(early[6], early[1]), master_down, avg_down, sq_down, 1, master_down_out, 160)
        master_up_out, own_three = apply_update(factor(early[4], early[2]), master_up, avg_up, sq_up, 1, None, 32)
        master_up_out, own_one = apply_update(factor(early[3], late[0]), master_up, avg_up, sq_up, 0, master_up_out, 32)
        new_four, new_three = gather_rows([own_four, own_three], n, 4)
        own_one, new_four, new_three = lax.optimization_barrier((own_one, new_four, new_three))
        new_one = gather(own_one)
        new_down = place(new_four, 1, place(new_two, 0, None, 640), 640)
        new_up = place(new_one, 0, place(new_three, 1, None, 128), 128)
        return (new_up, new_down, master_up_out, master_down_out, avg_up, avg_down, sq_up, sq_down, grad_norm)


    return jax.shard_map(device_body, mesh=mesh, in_specs=(batch_rows, batch_rows, replicated, replicated, state_rows, state_rows, state_rows, state_rows, state_rows, state_rows, replicated, replicated), out_specs=(replicated, replicated, state_rows, state_rows, state_rows, state_rows, state_rows, state_rows, replicated), check_vma=False)
```
